32 devices in a mesh: rows: 8 (over z, x), cols: 4 (over y, core).
Axes of the slice: x: 2, y: 2, z: 4, core: 2. Of those that a mesh axis runs over, the one named last changes fastest.
Arguments:
- lattice: int32 [256, 16384], P('rows', 'cols'), may hold values from -1 to 1, as said below
- draws: int32 [2, 256, 16384], P(None, 'rows', 'cols'), may hold values from -2147483648 to 2147483647, as said below
- thresholds: int32 [5], replicated, may hold values from 32 to 256
Outputs:
- final_lattice: int32 [256, 16384], P('rows', 'cols')
- row_magnetization: float32 [256], P('rows')
The draws below stay inside these ranges and needn't reach their ends.
Inputs may be any that keep to these rules, and one draw needn't show every extreme that they name: `lattice`: every entry is -1 or 1. Each word holds four independent draws of 0 to 255: bits 8k to 8k+7 of draws[p] belong to sweep 4p + k.
All inputs are finite; a program needn't handle non-finite values.
Results may differ from the reference program's by a relative error of at most 0.0003.
Values sent between devices are 32-bit elements; how exact they have to be, the bound alone decides.
A program may use at most 64 MiB of HBM per device.

```python
import jax
import jax.numpy as jnp
from jax import lax

SWEEPS = 8
LEVELS = 5
NX = 256
NY = 16384
PACKS = 2


def draw_lattice(key, part):
    picks = jax.random.randint(jax.random.fold_in(key, 11), (NX, NY), 0, 20 * NX, dtype=jnp.int32)
    row_ids = lax.broadcasted_iota(jnp.int32, (NX, NY), 0)
    return jnp.where(picks < 11 * NX + 8 * row_ids, 1, -1).astype(jnp.int32)


def draw_draws(key, part):
    return jax.random.randint(jax.random.fold_in(key, 23), (PACKS, NX, NY), -2147483648, 2147483647, dtype=jnp.int32)


def plant(entries, own_key, least, top_value):
    shape = entries.shape
    spot = [jax.random.randint(jax.random.fold_in(own_key, axis), (), 0, shape[axis]) for axis in range(len(shape))]
    entries = entries.at[tuple(spot)].set(least)
    longest = shape.index(max(shape))
    spot[longest] = (spot[longest] + 1) % shape[longest]
    return entries.at[tuple(spot)].set(top_value)


def setup_inputs(seed: int = 0) -> dict:
    splits = jax.random.split(jax.random.key(seed), 4)
    lattice = draw_lattice(jax.random.fold_in(splits[3], 71), 0)
    draws = draw_draws(jax.random.fold_in(splits[3], 71), 0)
    thresholds = plant(jax.random.randint(splits[2], (LEVELS,), 32, 257), jax.random.fold_in(splits[2], 1), 32, 256).astype(jnp.int32)
    return dict(lattice=lattice, draws=draws, thresholds=thresholds)


def reference(lattice, draws, thresholds):
    spins_now = lattice
    row_ids = lax.broadcasted_iota(jnp.int32, lattice.shape, 0)
    col_ids = lax.broadcasted_iota(jnp.int32, lattice.shape, 1)
    parity = (row_ids + col_ids) % 2
    for sweep_no in range(SWEEPS):
        draw_bytes = (draws[sweep_no // 4] >> (8 * (sweep_no % 4))) & 255
        for colour in (0, 1):
            neighbours = (jnp.roll(spins_now, 1, 0) + jnp.roll(spins_now, -1, 0)
                          + jnp.roll(spins_now, 1, 1) + jnp.roll(spins_now, -1, 1))
            level = (spins_now * neighbours + 4) // 2
            allowed = jnp.zeros_like(spins_now)
            for entry in range(LEVELS):
                allowed = jnp.where(level == entry, thresholds[entry], allowed)
            flipped = (parity == colour) & (draw_bytes < allowed)
            spins_now = jnp.where(flipped, -spins_now, spins_now)
    means = jnp.sum(spins_now.astype(jnp.float32), axis=1) / NY
    return spins_now, means
```

```python
import functools

import jax
import jax.numpy as jnp
from jax import lax
from jax.experimental import pallas as pl
from jax.experimental.pallas import tpu as pltpu
from jax.sharding import PartitionSpec as P

SWEEPS = 8
LEVELS = 5
PER_WORD = 4
BITS = 8
DEPTH = 8
LANES = 128
WORD = 32
MESH = pl.DeviceIdType.MESH

shr = lax.shift_right_logical


def transposed(words):
    words = list(words)
    mask = 0x0000FFFF
    j = 16
    while j:
        signed = mask - (1 << 32) if mask >> 31 else mask
        for k in range(WORD):
            if k & j:
                continue
            low, high = words[k], words[k + j]
            t = (shr(low, jnp.int32(j)) ^ high) & jnp.int32(signed)
            words[k + j] = high ^ t
            words[k] = low ^ (t << j)
        j >>= 1
        mask = (mask ^ (mask << j)) & 0xFFFFFFFF
    return words


def accept_masks(planes, bit_masks):
    below = []
    for level in range(LEVELS):
        t = bit_masks[level]
        z = planes[0] & t[0]
        for b in range(1, BITS):
            z = (z ^ (t[b - 1] ^ t[b])) & (planes[b] ^ ~t[b])
        below.append((z ^ t[BITS - 1]) | t[BITS])
    return below[0], below[0] ^ below[1], below[2], below[2] ^ below[3], below[0] ^ below[4]


def lane_neighbours(main, side, lane):
    rm, rs = pltpu.roll(main, 1, 1), pltpu.roll(side, 1, 1)
    sm, ss = pltpu.roll(main, LANES - 1, 1), pltpu.roll(side, LANES - 1, 1)
    first, last = lane == 0, lane == LANES - 1
    left_m = jnp.where(first, (rm << 1) | (rs & 1), rm)
    left_s = jnp.where(first, shr(rm, jnp.int32(30)) & 2, rs)
    right_m = jnp.where(last, shr(sm, jnp.int32(1)) | ((ss & 2) << 30), sm)
    right_s = jnp.where(last, sm & 1, ss)
    return (left_m, right_m), (left_s, right_s)


def updated(word, across, accept, colour_mask):
    rows = word.shape[0]
    a0, d1, a2, d3, d4 = accept
    x1, x2 = pltpu.roll(word, 1, 0) ^ word, pltpu.roll(word, rows - 1, 0) ^ word
    x3, x4 = across[0] ^ word, across[1] ^ word
    p, c1 = x1 ^ x2, ~(x1 | x2)
    q, c2 = x3 ^ x4, ~(x3 | x4)
    ones, twos, fours = p ^ q, (c1 ^ c2) | (p & q), c1 & c2
    low, high = a0 ^ (ones & d1), a2 ^ (ones & d3)
    take = low ^ (twos & (low ^ high)) ^ (fours & d4)
    return word ^ (take & colour_mask)


def sweep_kernel(shape, lat_ref, draws_ref, thr_ref, word_ref, mean_ref,
                 spins, draws, accept, state, out_edge, in_edge, count, peers,
                 local_sem, send_sem, recv_sem, edge_send, edge_recv, peer_send, peer_recv):
    n_rows, n_cols = shape
    rows, cols = lat_ref.shape
    tiles = cols // LANES
    packs = draws_ref.shape[0]
    ext = rows + 2 * DEPTH
    r, c = lax.axis_index("rows"), lax.axis_index("cols")
    up, down = lax.rem(r + n_rows - 1, n_rows), lax.rem(r + 1, n_rows)
    left, right = lax.rem(c + n_cols - 1, n_cols), lax.rem(c + 1, n_cols)

    local = [pltpu.make_async_copy(lat_ref, spins.at[pl.ds(DEPTH, rows), pl.ds(0, cols)], local_sem.at[0])]
    for pack in range(packs):
        local.append(pltpu.make_async_copy(
            draws_ref.at[pack], draws.at[pack, pl.ds(DEPTH, rows), pl.ds(0, cols)], local_sem.at[1 + pack]))
    for copy in local:
        copy.start()

    barrier = pltpu.get_barrier_semaphore()
    around = [(a, b) for a in (up, r, down) for b in (left, c, right)]
    del around[4]
    others = [lax.rem(c + k, n_cols) for k in range(1, n_cols)]
    for target in around + [(r, b) for b in others[1:-1]]:
        pl.semaphore_signal(barrier, inc=1, device_id=target, device_id_type=MESH)
    pl.semaphore_wait(barrier, len(around) + n_cols - 3)

    row_part = {-1: (0, DEPTH, DEPTH + rows), 0: (0, rows, DEPTH), 1: (rows - DEPTH, DEPTH, 0)}
    col_part = {-1: (0, LANES, cols + LANES), 0: (0, cols, 0), 1: (cols - LANES, LANES, cols)}
    row_id = {-1: up, 0: r, 1: down}
    col_id = {-1: left, 0: c, 1: right}
    sides = [(-1, 0), (1, 0), (0, -1), (0, 1), (-1, -1), (-1, 1), (1, -1), (1, 1)]
    first, later = [], []
    for stage in range(1 + packs):
        for index, (dr, dc) in enumerate(sides):
            r0, rn, rd = row_part[dr]
            c0, cn, cd = col_part[dc]
            src, dst = (lat_ref, spins) if stage == 0 else (draws_ref.at[stage - 1], draws.at[stage - 1])
            copy = pltpu.make_async_remote_copy(
                src_ref=src.at[pl.ds(r0, rn), pl.ds(c0, cn)],
                dst_ref=dst.at[pl.ds(rd, rn), pl.ds(cd, cn)],
                send_sem=send_sem.at[stage, index],
                recv_sem=recv_sem.at[stage, index],
                device_id=(row_id[dr], col_id[dc]),
                device_id_type=MESH,
            )
            copy.start()
            (first if stage <= 1 else later).append(copy)

    bit_masks = []
    for level in range(LEVELS):
        t = thr_ref[level]
        bit_masks.append([-((t >> b) & 1) for b in range(BITS + 1)])

    def tile_of(ref, row0, b):
        return ref[pl.ds(row0, 8), pl.ds(b * LANES, LANES)]

    def prepare(pack, group):
        row0 = pl.multiple_of(group * 8, 8)
        source = draws.at[pack]
        planes = transposed([tile_of(source, row0, b) for b in range(tiles)])
        for t in range(PER_WORD):
            masks = accept_masks(planes[BITS * t:BITS * (t + 1)], bit_masks)
            for k in range(LEVELS):
                accept[pack * PER_WORD + t, k, 0, pl.ds(row0, 8), :] = masks[k]

    def prepare_side(pack, group):
        row0 = pl.multiple_of(group * 8, 8)
        source = draws.at[pack]
        lo, hi = tile_of(source, row0, tiles), tile_of(source, row0, tiles + 1)
        even = (lo & 0x55555555) | ((hi & 0x55555555) << 1)
        odd = (shr(lo, jnp.int32(1)) & 0x55555555) | (hi & -0x55555556)
        planes = [shr((even, odd)[q & 1], jnp.int32(q & ~1)) for q in range(WORD)]
        for t in range(PER_WORD):
            masks = accept_masks(planes[BITS * t:BITS * (t + 1)], bit_masks)
            for k in range(LEVELS):
                accept[pack * PER_WORD + t, k, 1, pl.ds(row0, 8), :] = masks[k]

    def pack_group(group):
        row0 = pl.multiple_of(group * 8, 8)
        word = shr(tile_of(spins, row0, 0), jnp.int32(31))
        for b in range(1, tiles):
            word = word | (tile_of(spins, row0, b) & jnp.int32(-(1 << 31) if b == 31 else 1 << b))
        state[0, pl.ds(row0, 8), :] = word

    def pack_side(group):
        row0 = pl.multiple_of(group * 8, 8)
        state[1, pl.ds(row0, 8), :] = shr(tile_of(spins, row0, tiles), jnp.int32(31)) | (
            tile_of(spins, row0, tiles + 1) & 2)

    groups = rows // 8
    halo = DEPTH // 8

    for copy in local:
        copy.wait()

    @pl.loop(halo, halo + groups)
    def _(group):
        pack_group(group)

    @pl.loop(0, packs * groups)
    def _(step):
        prepare(step // groups, halo + step % groups)

    for copy in first:
        copy.wait()

    @pl.loop(halo, halo + groups)
    def _(group):
        pack_side(group)

    for group in (0, halo + groups):
        pack_group(group)
        pack_side(group)

    @pl.loop(0, 2)
    def _(side):
        prepare(0, side * (halo + groups))

    @pl.loop(0, groups + 2 * halo)
    def _(group):
        prepare_side(0, group)

    lane = lax.broadcasted_iota(jnp.int32, (ext, LANES), 1)
    base = r * rows + c * cols - DEPTH
    site = lax.broadcasted_iota(jnp.int32, (ext, LANES), 0) + lane + base
    odd_sites = -(site & 1)

    def sweep(sweep_no):
        main, side = state[0], state[1]
        for colour_mask in (~odd_sites, odd_sites):
            across_m, across_s = lane_neighbours(main, side, lane)
            main, side = (
                updated(main, across_m, [accept[sweep_no, k, 0] for k in range(LEVELS)], colour_mask),
                updated(side, across_s, [accept[sweep_no, k, 1] for k in range(LEVELS)], colour_mask),
            )
        state[0] = main
        state[1] = side

    half = DEPTH // 2

    @pl.loop(0, half)
    def _(t):
        sweep(t)

    copies = []
    for index, (row0, dev) in enumerate(((DEPTH, up), (rows, down))):
        main, side = state[0, pl.ds(row0, DEPTH), :], state[1, pl.ds(row0, DEPTH), :]
        for b in range(tiles):
            out_edge[index, :, pl.ds(b * LANES, LANES)] = shr(main, jnp.int32(b)) & 1
        for b in range(2):
            out_edge[index, :, pl.ds(cols + b * LANES, LANES)] = shr(side, jnp.int32(b)) & 1
        copy = pltpu.make_async_remote_copy(
            src_ref=out_edge.at[index],
            dst_ref=in_edge.at[index],
            send_sem=edge_send.at[index],
            recv_sem=edge_recv.at[index],
            device_id=(dev, c),
            device_id_type=MESH,
        )
        copy.start()
        copies.append(copy)

    for copy in later:
        copy.wait()

    @pl.loop(0, 2)
    def _(side):
        prepare(1, side * (halo + groups))

    @pl.loop(0, groups + 2 * halo)
    def _(group):
        prepare_side(1, group)

    for index, (row0, copy) in enumerate(((DEPTH + rows, copies[0]), (0, copies[1]))):
        copy.wait()
        word = in_edge[index, :, pl.ds(0, LANES)]
        for b in range(1, tiles):
            word = word | (in_edge[index, :, pl.ds(b * LANES, LANES)] << b)
        state[0, pl.ds(row0, DEPTH), :] = word
        state[1, pl.ds(row0, DEPTH), :] = in_edge[index, :, pl.ds(cols, LANES)] | (
            in_edge[index, :, pl.ds(cols + LANES, LANES)] << 1)

    @pl.loop(half, SWEEPS)
    def _(t):
        sweep(t)

    final = state[0, pl.ds(DEPTH, rows), :]
    word_ref[...] = final
    count[...] = lax.population_count(final)
    copies = []
    for k in range(1, n_cols):
        copy = pltpu.make_async_remote_copy(
            src_ref=count,
            dst_ref=peers.at[k - 1],
            send_sem=peer_send.at[k - 1],
            recv_sem=peer_recv.at[k - 1],
            device_id=(r, others[k - 1]),
            device_id_type=MESH,
        )
        copy.start()
        copies.append(copy)
    total = count[...]
    for k in range(1, n_cols):
        copies[k - 1].wait()
        total = total + peers[k - 1]
    downs = jnp.sum(total.astype(jnp.float32), axis=1, keepdims=True)
    width = n_cols * cols
    mean = (width - 2.0 * downs) / width
    at = lax.broadcasted_iota(jnp.int32, (rows, LANES), 0) == lax.broadcasted_iota(jnp.int32, (rows, LANES), 1)
    mean_ref[...] = jnp.sum(jnp.where(at, mean, 0.0), axis=0, keepdims=True)


def unpack_kernel(word_ref, row_ref, lattice_ref, mean_ref):
    word = word_ref[...]
    for b in range(lattice_ref.shape[1] // LANES):
        lattice_ref[:, b * LANES:(b + 1) * LANES] = 1 - ((shr(word, jnp.int32(b)) & 1) << 1)
    mean_ref[...] = row_ref[...]


def on_device(shape, lattice, draws, thresholds):
    rows, cols = lattice.shape
    packs = draws.shape[0]
    assert cols == WORD * LANES and rows <= LANES and rows % 8 == 0 and 2 * DEPTH == 2 * SWEEPS
    ext, wide = rows + 2 * DEPTH, cols + 2 * LANES
    n_cols = shape[1]
    vmem, hbm = pltpu.VMEM, pl.ANY
    word, mean = pl.pallas_call(
        functools.partial(sweep_kernel, shape),
        out_shape=(
            jax.ShapeDtypeStruct((rows, LANES), jnp.int32),
            jax.ShapeDtypeStruct((1, LANES), jnp.float32),
        ),
        in_specs=[
            pl.BlockSpec(memory_space=hbm),
            pl.BlockSpec(memory_space=hbm),
            pl.BlockSpec(memory_space=pltpu.SMEM),
        ],
        out_specs=(pl.BlockSpec(memory_space=vmem), pl.BlockSpec(memory_space=vmem)),
        scratch_shapes=[
            vmem((ext, wide), jnp.int32),
            vmem((packs, ext, wide), jnp.int32),
            vmem((SWEEPS, LEVELS, 2, ext, LANES), jnp.int32),
            vmem((2, ext, LANES), jnp.int32),
            vmem((2, DEPTH, wide), jnp.int32),
            vmem((2, DEPTH, wide), jnp.int32),
            vmem((rows, LANES), jnp.int32),
            vmem((n_cols - 1, rows, LANES), jnp.int32),
            pltpu.SemaphoreType.DMA((1 + packs,)),
            pltpu.SemaphoreType.DMA((1 + packs, 8)),
            pltpu.SemaphoreType.DMA((1 + packs, 8)),
            pltpu.SemaphoreType.DMA((2,)),
            pltpu.SemaphoreType.DMA((2,)),
            pltpu.SemaphoreType.DMA((n_cols - 1,)),
            pltpu.SemaphoreType.DMA((n_cols - 1,)),
        ],
        compiler_params=pltpu.CompilerParams(collective_id=0, has_side_effects=True),
        name="sweeps",
    )(lattice, draws, thresholds)
    final, means = pl.pallas_call(
        unpack_kernel,
        out_shape=(
            jax.ShapeDtypeStruct((rows, cols), jnp.int32),
            jax.ShapeDtypeStruct((1, LANES), jnp.float32),
        ),
        name="unpack",
    )(word, mean)
    return final, means[0, :rows]


def solution(mesh):
    shape = (mesh.shape["rows"], mesh.shape["cols"])
    in_specs = (P("rows", "cols"), P(None, "rows", "cols"), P())
    out_specs = (P("rows", "cols"), P("rows"))
    return jax.shard_map(
        functools.partial(on_device, shape), mesh=mesh, in_specs=in_specs, out_specs=out_specs, check_vma=False
    )
```

```python
import functools

import jax
import jax.numpy as jnp
from jax import lax
from jax.experimental import pallas as pl
from jax.experimental.pallas import tpu as pltpu
from jax.sharding import PartitionSpec as P

SWEEPS = 8
LEVELS = 5
PER_WORD = 4
BITS = 8
DEPTH = 8
LANES = 128
WORD = 32
MESH = pl.DeviceIdType.MESH

shr = lax.shift_right_logical


def transposed(words):
    words = list(words)
    mask = 0x0000FFFF
    j = 16
    while j:
        signed = mask - (1 << 32) if mask >> 31 else mask
        for k in range(WORD):
            if k & j:
                continue
            low, high = words[k], words[k + j]
            t = (shr(low, jnp.int32(j)) ^ high) & jnp.int32(signed)
            words[k + j] = high ^ t
            words[k] = low ^ (t << j)
        j >>= 1
        mask = (mask ^ (mask << j)) & 0xFFFFFFFF
    return words


def accept_masks(planes, bit_masks):
    below = []
    for level in range(LEVELS):
        t = bit_masks[level]
        z = planes[0] & t[0]
        for b in range(1, BITS):
            z = (z ^ (t[b - 1] ^ t[b])) & (planes[b] ^ ~t[b])
        below.append((z ^ t[BITS - 1]) | t[BITS])
    return below[0], below[0] ^ below[1], below[2], below[2] ^ below[3], below[0] ^ below[4]


def lane_neighbours(main, side, lane):
    rm, rs = pltpu.roll(main, 1, 1), pltpu.roll(side, 1, 1)
    sm, ss = pltpu.roll(main, LANES - 1, 1), pltpu.roll(side, LANES - 1, 1)
    first, last = lane == 0, lane == LANES - 1
    left_m = jnp.where(first, (rm << 1) | (rs & 1), rm)
    left_s = jnp.where(first, shr(rm, jnp.int32(30)) & 2, rs)
    right_m = jnp.where(last, shr(sm, jnp.int32(1)) | ((ss & 2) << 30), sm)
    right_s = jnp.where(last, sm & 1, ss)
    return (left_m, right_m), (left_s, right_s)


def updated(word, across, accept, colour_mask):
    rows = word.shape[0]
    a0, d1, a2, d3, d4 = accept
    x1, x2 = pltpu.roll(word, 1, 0) ^ word, pltpu.roll(word, rows - 1, 0) ^ word
    x3, x4 = across[0] ^ word, across[1] ^ word
    p, c1 = x1 ^ x2, ~(x1 | x2)
    q, c2 = x3 ^ x4, ~(x3 | x4)
    ones, twos, fours = p ^ q, (c1 ^ c2) | (p & q), c1 & c2
    low, high = a0 ^ (ones & d1), a2 ^ (ones & d3)
    take = low ^ (twos & (low ^ high)) ^ (fours & d4)
    return word ^ (take & colour_mask)


def sweep_kernel(shape, lat_ref, draws_ref, thr_ref, word_ref, mean_ref,
                 spins, draws, accept, state, out_edge, in_edge, count, peers,
                 local_sem, send_sem, recv_sem, edge_send, edge_recv, peer_send, peer_recv):
    n_rows, n_cols = shape
    rows, cols = lat_ref.shape
    tiles = cols // LANES
    packs = draws_ref.shape[0]
    ext = rows + 2 * DEPTH
    r, c = lax.axis_index("rows"), lax.axis_index("cols")
    up, down = lax.rem(r + n_rows - 1, n_rows), lax.rem(r + 1, n_rows)
    left, right = lax.rem(c + n_cols - 1, n_cols), lax.rem(c + 1, n_cols)

    local = [pltpu.make_async_copy(lat_ref, spins.at[pl.ds(DEPTH, rows), pl.ds(0, cols)], local_sem.at[0])]
    for pack in range(packs):
        local.append(pltpu.make_async_copy(
            draws_ref.at[pack], draws.at[pack, pl.ds(DEPTH, rows), pl.ds(0, cols)], local_sem.at[1 + pack]))
    for copy in local:
        copy.start()

    barrier = pltpu.get_barrier_semaphore()
    around = [(a, b) for a in (up, r, down) for b in (left, c, right)]
    del around[4]
    others = [lax.rem(c + k, n_cols) for k in range(1, n_cols)]
    for target in around + [(r, b) for b in others[1:-1]]:
        pl.semaphore_signal(barrier, inc=1, device_id=target, device_id_type=MESH)
    pl.semaphore_wait(barrier, len(around) + n_cols - 3)

    def row_part(depth):
        return {-1: (0, depth, DEPTH + rows), 0: (0, rows, DEPTH), 1: (rows - depth, depth, DEPTH - depth)}

    col_part = {-1: (0, LANES, cols + LANES), 0: (0, cols, 0), 1: (cols - LANES, LANES, cols)}
    row_id = {-1: up, 0: r, 1: down}
    col_id = {-1: left, 0: c, 1: right}
    sides = [(0, -1), (0, 1), (-1, -1), (-1, 1), (1, -1), (1, 1), (-1, 0), (1, 0)]
    strips, first, later = [], [], []

    def send(stage, index):
        dr, dc = sides[index]
        r0, rn, rd = row_part(DEPTH - min(stage, 1))[dr]
        c0, cn, cd = col_part[dc]
        src, dst = (lat_ref, spins) if stage == 0 else (draws_ref.at[stage - 1], draws.at[stage - 1])
        copy = pltpu.make_async_remote_copy(
            src_ref=src.at[pl.ds(r0, rn), pl.ds(c0, cn)],
            dst_ref=dst.at[pl.ds(rd, rn), pl.ds(cd, cn)],
            send_sem=send_sem.at[stage, index],
            recv_sem=recv_sem.at[stage, index],
            device_id=(row_id[dr], col_id[dc]),
            device_id_type=MESH,
        )
        copy.start()
        return copy

    for stage in range(1 + packs):
        strips += [send(stage, index) for index in (0, 1)]
    for stage in range(1 + packs):
        copies = [send(stage, index) for index in range(2, len(sides))]
        if stage <= 1:
            first += copies
        else:
            later += copies

    bit_masks = []
    for level in range(LEVELS):
        t = thr_ref[level]
        bit_masks.append([-((t >> b) & 1) for b in range(BITS + 1)])

    def tile_of(ref, row0, b):
        return ref[pl.ds(row0, 8), pl.ds(b * LANES, LANES)]

    def prepare(pack, group):
        row0 = pl.multiple_of(group * 8, 8)
        source = draws.at[pack]
        planes = transposed([tile_of(source, row0, b) for b in range(tiles)])
        for t in range(PER_WORD):
            masks = accept_masks(planes[BITS * t:BITS * (t + 1)], bit_masks)
            for k in range(LEVELS):
                accept[pack * PER_WORD + t, k, 0, pl.ds(row0, 8), :] = masks[k]

    def prepare_side(pack, group):
        row0 = pl.multiple_of(group * 8, 8)
        source = draws.at[pack]
        lo, hi = tile_of(source, row0, tiles), tile_of(source, row0, tiles + 1)
        even = (lo & 0x55555555) | ((hi & 0x55555555) << 1)
        odd = (shr(lo, jnp.int32(1)) & 0x55555555) | (hi & -0x55555556)
        planes = [shr((even, odd)[q & 1], jnp.int32(q & ~1)) for q in range(WORD)]
        for t in range(PER_WORD):
            masks = accept_masks(planes[BITS * t:BITS * (t + 1)], bit_masks)
            for k in range(LEVELS):
                accept[pack * PER_WORD + t, k, 1, pl.ds(row0, 8), :] = masks[k]

    def pack_group(group):
        row0 = pl.multiple_of(group * 8, 8)
        word = shr(tile_of(spins, row0, 0), jnp.int32(31))
        for b in range(1, tiles):
            word = word | (tile_of(spins, row0, b) & jnp.int32(-(1 << 31) if b == 31 else 1 << b))
        state[0, pl.ds(row0, 8), :] = word

    def pack_side(group):
        row0 = pl.multiple_of(group * 8, 8)
        state[1, pl.ds(row0, 8), :] = shr(tile_of(spins, row0, tiles), jnp.int32(31)) | (
            tile_of(spins, row0, tiles + 1) & 2)

    groups = rows // 8
    halo = DEPTH // 8

    for copy in local:
        copy.wait()

    @pl.loop(halo, halo + groups)
    def _(group):
        pack_group(group)

    @pl.loop(0, packs * groups)
    def _(step):
        prepare(step // groups, halo + step % groups)

    for copy in strips:
        copy.wait()

    @pl.loop(halo, halo + groups)
    def _(group):
        pack_side(group)

    @pl.loop(0, packs * groups)
    def _(step):
        prepare_side(step // groups, halo + step % groups)

    for copy in first:
        copy.wait()

    for group in (0, halo + groups):
        pack_group(group)
        pack_side(group)

    @pl.loop(0, 2)
    def _(side):
        prepare(0, side * (halo + groups))
        prepare_side(0, side * (halo + groups))

    lane = lax.broadcasted_iota(jnp.int32, (ext, LANES), 1)
    base = r * rows + c * cols - DEPTH
    site = lax.broadcasted_iota(jnp.int32, (ext, LANES), 0) + lane + base
    odd_sites = -(site & 1)

    def sweep(sweep_no):
        main, side = state[0], state[1]
        for colour_mask in (~odd_sites, odd_sites):
            across_m, across_s = lane_neighbours(main, side, lane)
            main, side = (
                updated(main, across_m, [accept[sweep_no, k, 0] for k in range(LEVELS)], colour_mask),
                updated(side, across_s, [accept[sweep_no, k, 1] for k in range(LEVELS)], colour_mask),
            )
        state[0] = main
        state[1] = side

    half = DEPTH // 2

    @pl.loop(0, half)
    def _(t):
        sweep(t)

    copies = []
    tile_id = lax.broadcasted_iota(jnp.int32, (WORD, LANES), 0)
    sub, lane8 = (lax.broadcasted_iota(jnp.int32, (DEPTH, LANES), d) for d in (0, 1))
    low_lanes = lane8 < LANES // 2
    near, far = (0, DEPTH - 1), (DEPTH - 1, 0)
    for index, (row0, dev) in enumerate(((DEPTH, up), (rows, down))):
        main, side = state[0, pl.ds(row0, DEPTH), :], state[1, pl.ds(row0, DEPTH), :]
        odd = odd_sites[row0:row0 + DEPTH]
        joint = (main & odd) | (pltpu.roll(main, 1 if index == 0 else DEPTH - 1, 0) & ~odd)
        main = jnp.where(sub == near[index], joint, main)
        for i in range(DEPTH - 1):
            row = main[i + index:i + index + 1]
            out_edge[index, pl.ds(i * WORD, WORD), :] = shr(jnp.broadcast_to(row, (WORD, LANES)), tile_id) & 1
        out_edge[index, pl.ds((DEPTH - 1) * WORD, DEPTH), :] = jnp.where(low_lanes, shr(side, jnp.int32(1)), side) & 1
        copy = pltpu.make_async_remote_copy(
            src_ref=out_edge.at[index],
            dst_ref=in_edge.at[index],
            send_sem=edge_send.at[index],
            recv_sem=edge_recv.at[index],
            device_id=(dev, c),
            device_id_type=MESH,
        )
        copy.start()
        copies.append(copy)

    for copy in later:
        copy.wait()

    @pl.loop(0, 2)
    def _(side):
        prepare(1, side * (halo + groups))
        prepare_side(1, side * (halo + groups))

    for index, (row0, copy) in enumerate(((DEPTH + rows, copies[0]), (0, copies[1]))):
        copy.wait()
        old = state[0, pl.ds(row0, DEPTH), :]
        odd = odd_sites[row0:row0 + DEPTH]
        word = old
        for i in range(DEPTH - 1):
            bits = in_edge[index, pl.ds(i * WORD, WORD), :] << tile_id
            row = bits[0:8] | bits[8:16] | bits[16:24] | bits[24:32]
            for shift in (4, 2, 1):
                row = row | pltpu.roll(row, shift, 0)
            at = i + index
            if at == near[index]:
                word = jnp.where(sub == far[index], row, word)
                row = (old & ~odd) | (row & odd)
            word = jnp.where(sub == at, row, word)
        state[0, pl.ds(row0, DEPTH), :] = word
        bits = in_edge[index, pl.ds((DEPTH - 1) * WORD, DEPTH), :]
        state[1, pl.ds(row0, DEPTH), :] = jnp.where(low_lanes, bits << 1, bits)

    @pl.loop(half, SWEEPS)
    def _(t):
        sweep(t)

    final = state[0, pl.ds(DEPTH, rows), :]
    word_ref[...] = final
    count[...] = lax.population_count(final)
    copies = []
    for k in range(1, n_cols):
        copy = pltpu.make_async_remote_copy(
            src_ref=count,
            dst_ref=peers.at[k - 1],
            send_sem=peer_send.at[k - 1],
            recv_sem=peer_recv.at[k - 1],
            device_id=(r, others[k - 1]),
            device_id_type=MESH,
        )
        copy.start()
        copies.append(copy)
    total = count[...]
    for k in range(1, n_cols):
        copies[k - 1].wait()
        total = total + peers[k - 1]
    downs = jnp.sum(total.astype(jnp.float32), axis=1, keepdims=True)
    width = n_cols * cols
    mean = (width - 2.0 * downs) / width
    at = lax.broadcasted_iota(jnp.int32, (rows, LANES), 0) == lax.broadcasted_iota(jnp.int32, (rows, LANES), 1)
    mean_ref[...] = jnp.sum(jnp.where(at, mean, 0.0), axis=0, keepdims=True)


def unpack_kernel(word_ref, row_ref, lattice_ref, mean_ref):
    word = word_ref[...]
    for b in range(lattice_ref.shape[1] // LANES):
        lattice_ref[:, b * LANES:(b + 1) * LANES] = 1 - ((shr(word, jnp.int32(b)) & 1) << 1)
    mean_ref[...] = row_ref[0, :mean_ref.shape[0]]


def on_device(shape, lattice, draws, thresholds):
    rows, cols = lattice.shape
    packs = draws.shape[0]
    assert cols == WORD * LANES and rows <= LANES and rows % 8 == 0 and 2 * DEPTH == 2 * SWEEPS
    ext, wide = rows + 2 * DEPTH, cols + 2 * LANES
    n_cols = shape[1]
    vmem, hbm = pltpu.VMEM, pl.ANY
    word, mean = pl.pallas_call(
        functools.partial(sweep_kernel, shape),
        out_shape=(
            jax.ShapeDtypeStruct((rows, LANES), jnp.int32),
            jax.ShapeDtypeStruct((1, LANES), jnp.float32),
        ),
        in_specs=[
            pl.BlockSpec(memory_space=hbm),
            pl.BlockSpec(memory_space=hbm),
            pl.BlockSpec(memory_space=pltpu.SMEM),
        ],
        out_specs=(pl.BlockSpec(memory_space=vmem), pl.BlockSpec(memory_space=vmem)),
        scratch_shapes=[
            vmem((ext, wide), jnp.int32),
            vmem((packs, ext, wide), jnp.int32),
            vmem((SWEEPS, LEVELS, 2, ext, LANES), jnp.int32),
            vmem((2, ext, LANES), jnp.int32),
            vmem((2, (DEPTH - 1) * WORD + DEPTH, LANES), jnp.int32),
            vmem((2, (DEPTH - 1) * WORD + DEPTH, LANES), jnp.int32),
            vmem((rows, LANES), jnp.int32),
            vmem((n_cols - 1, rows, LANES), jnp.int32),
            pltpu.SemaphoreType.DMA((1 + packs,)),
            pltpu.SemaphoreType.DMA((1 + packs, 8)),
            pltpu.SemaphoreType.DMA((1 + packs, 8)),
            pltpu.SemaphoreType.DMA((2,)),
            pltpu.SemaphoreType.DMA((2,)),
            pltpu.SemaphoreType.DMA((n_cols - 1,)),
            pltpu.SemaphoreType.DMA((n_cols - 1,)),
        ],
        compiler_params=pltpu.CompilerParams(collective_id=0, has_side_effects=True),
        name="sweeps",
    )(lattice, draws, thresholds)
    final, means = pl.pallas_call(
        unpack_kernel,
        out_shape=(
            jax.ShapeDtypeStruct((rows, cols), jnp.int32),
            jax.ShapeDtypeStruct((rows,), jnp.float32),
        ),
        name="unpack",
    )(word, mean)
    return final, means


def solution(mesh):
    shape = (mesh.shape["rows"], mesh.shape["cols"])
    in_specs = (P("rows", "cols"), P(None, "rows", "cols"), P())
    out_specs = (P("rows", "cols"), P("rows"))
    return jax.shard_map(
        functools.partial(on_device, shape), mesh=mesh, in_specs=in_specs, out_specs=out_specs, check_vma=False
    )
```

```python
import functools

import jax
import jax.numpy as jnp
from jax import lax
from jax.experimental import pallas as pl
from jax.experimental.pallas import tpu as pltpu
from jax.sharding import PartitionSpec as P

SWEEPS = 8
LEVELS = 5
PER_WORD = 4
BITS = 8
DEPTHS = (4, 4, 4, 4)
HALO = 8
LANES = 128
WORD = 32
MESH = pl.DeviceIdType.MESH

shr = lax.shift_right_logical


def transposed(words):
    words = list(words)
    mask = 0x0000FFFF
    j = 16
    while j:
        signed = mask - (1 << 32) if mask >> 31 else mask
        for k in range(WORD):
            if k & j:
                continue
            low, high = words[k], words[k + j]
            t = (shr(low, jnp.int32(j)) ^ high) & jnp.int32(signed)
            words[k + j] = high ^ t
            words[k] = low ^ (t << j)
        j >>= 1
        mask = (mask ^ (mask << j)) & 0xFFFFFFFF
    return words


def accept_masks(planes, bit_masks):
    below = []
    for level in range(LEVELS):
        t = bit_masks[level]
        z = planes[0] & t[0]
        for b in range(1, BITS):
            z = (z ^ (t[b - 1] ^ t[b])) & (planes[b] ^ ~t[b])
        below.append((z ^ t[BITS - 1]) | t[BITS])
    return below[0], below[0] ^ below[1], below[2], below[2] ^ below[3], below[0] ^ below[4]


def lane_neighbours(main, side, lane):
    rm, rs = pltpu.roll(main, 1, 1), pltpu.roll(side, 1, 1)
    sm, ss = pltpu.roll(main, LANES - 1, 1), pltpu.roll(side, LANES - 1, 1)
    first, last = lane == 0, lane == LANES - 1
    left_m = jnp.where(first, (rm << 1) | (rs & 1), rm)
    left_s = jnp.where(first, shr(rm, jnp.int32(30)) & 2, rs)
    right_m = jnp.where(last, shr(sm, jnp.int32(1)) | ((ss & 2) << 30), sm)
    right_s = jnp.where(last, sm & 1, ss)
    return (left_m, right_m), (left_s, right_s)


def updated(word, across, accept, colour_mask):
    rows = word.shape[0]
    a0, d1, a2, d3, d4 = accept
    x1, x2 = pltpu.roll(word, 1, 0) ^ word, pltpu.roll(word, rows - 1, 0) ^ word
    x3, x4 = across[0] ^ word, across[1] ^ word
    p, c1 = x1 ^ x2, ~(x1 | x2)
    q, c2 = x3 ^ x4, ~(x3 | x4)
    ones, twos, fours = p ^ q, (c1 ^ c2) | (p & q), c1 & c2
    low, high = a0 ^ (ones & d1), a2 ^ (ones & d3)
    take = low ^ (twos & (low ^ high)) ^ (fours & d4)
    return word ^ (take & colour_mask)


def sweep_kernel(shape, lat_ref, draws_ref, thr_ref, word_ref, mean_ref,
                 spins, draws, accept, state, out_edge, in_edge, count, peers,
                 local_sem, send_sem, recv_sem, edge_send, edge_recv, peer_send, peer_recv):
    n_rows, n_cols = shape
    rows, cols = lat_ref.shape
    tiles = cols // LANES
    packs = draws_ref.shape[0]
    ext = rows + 2 * HALO
    r, c = lax.axis_index("rows"), lax.axis_index("cols")
    up, down = lax.rem(r + n_rows - 1, n_rows), lax.rem(r + 1, n_rows)
    left, right = lax.rem(c + n_cols - 1, n_cols), lax.rem(c + 1, n_cols)

    local = [pltpu.make_async_copy(lat_ref, spins.at[pl.ds(HALO, rows), pl.ds(0, cols)], local_sem.at[0])]
    for pack in range(packs):
        local.append(pltpu.make_async_copy(
            draws_ref.at[pack], draws.at[pack, pl.ds(HALO, rows), pl.ds(0, cols)], local_sem.at[1 + pack]))
    for copy in local:
        copy.start()

    barrier = pltpu.get_barrier_semaphore()
    around = [(up, c), (down, c), (r, left), (r, right)]
    others = [lax.rem(c + k, n_cols) for k in range(1, n_cols)]
    for target in around + [(r, b) for b in others[1:-1]]:
        pl.semaphore_signal(barrier, inc=1, device_id=target, device_id_type=MESH)
    pl.semaphore_wait(barrier, len(around) + n_cols - 3)

    def row_part(depth):
        return {-1: (0, depth, HALO + rows), 0: (0, rows, HALO), 1: (rows - depth, depth, HALO - depth)}

    col_part = {-1: (0, LANES, cols + LANES), 0: (0, cols, 0), 1: (cols - LANES, LANES, cols)}
    row_id = {-1: up, 0: r, 1: down}
    col_id = {-1: left, 0: c, 1: right}
    sides = [(-1, 0), (1, 0), (0, -1), (0, 1)]
    done = [sum(DEPTHS[:turn + 1]) for turn in range(len(DEPTHS))]
    word_span = 2 * PER_WORD
    reach = [DEPTHS[0]] + [
        max(d for d, end in zip(DEPTHS, done) if end - d < word_span * (p + 1) and end > word_span * p) - 1
        for p in range(packs)
    ]

    def send(stage, index):
        dr, dc = sides[index]
        r0, rn, rd = row_part(reach[stage])[dr]
        c0, cn, cd = col_part[dc]
        src, dst = (lat_ref, spins) if stage == 0 else (draws_ref.at[stage - 1], draws.at[stage - 1])
        copy = pltpu.make_async_remote_copy(
            src_ref=src.at[pl.ds(r0, rn), pl.ds(c0, cn)],
            dst_ref=dst.at[pl.ds(rd, rn), pl.ds(cd, cn)],
            send_sem=send_sem.at[stage, index],
            recv_sem=recv_sem.at[stage, index],
            device_id=(row_id[dr], col_id[dc]),
            device_id_type=MESH,
        )
        copy.start()
        return copy

    def pass_on(stage, index):
        r0, rn, rd = row_part(reach[stage])[sides[index][0]]
        block = spins if stage == 0 else draws.at[stage - 1]
        copy = pltpu.make_async_remote_copy(
            src_ref=block.at[pl.ds(HALO + r0, rn), pl.ds(cols, 2 * LANES)],
            dst_ref=block.at[pl.ds(rd, rn), pl.ds(cols, 2 * LANES)],
            send_sem=send_sem.at[stage, 4 + index],
            recv_sem=recv_sem.at[stage, 4 + index],
            device_id=(row_id[sides[index][0]], c),
            device_id_type=MESH,
        )
        copy.start()
        return copy

    first = [send(stage, index) for stage in (0, 1) for index in (0, 1)]
    strips = [send(stage, index) for stage in range(1 + packs) for index in (2, 3)]

    bit_masks = []
    for level in range(LEVELS):
        t = thr_ref[level]
        bit_masks.append([-((t >> b) & 1) for b in range(BITS + 1)])

    def tile_of(ref, row0, b):
        return ref[pl.ds(row0, 8), pl.ds(b * LANES, LANES)]

    def prepare(pack, group):
        row0 = pl.multiple_of(group * 8, 8)
        source = draws.at[pack]
        planes = transposed([tile_of(source, row0, b) for b in range(tiles)])
        for t in range(PER_WORD):
            masks = accept_masks(planes[BITS * t:BITS * (t + 1)], bit_masks)
            for k in range(LEVELS):
                accept[pack * PER_WORD + t, k, 0, pl.ds(row0, 8), :] = masks[k]

    def prepare_side(pack, group):
        row0 = pl.multiple_of(group * 8, 8)
        source = draws.at[pack]
        lo, hi = tile_of(source, row0, tiles), tile_of(source, row0, tiles + 1)
        even = (lo & 0x55555555) | ((hi & 0x55555555) << 1)
        odd = (shr(lo, jnp.int32(1)) & 0x55555555) | (hi & -0x55555556)
        planes = [shr((even, odd)[q & 1], jnp.int32(q & ~1)) for q in range(WORD)]
        for t in range(PER_WORD):
            masks = accept_masks(planes[BITS * t:BITS * (t + 1)], bit_masks)
            for k in range(LEVELS):
                accept[pack * PER_WORD + t, k, 1, pl.ds(row0, 8), :] = masks[k]

    def pack_group(group):
        row0 = pl.multiple_of(group * 8, 8)
        word = shr(tile_of(spins, row0, 0), jnp.int32(31))
        for b in range(1, tiles):
            word = word | (tile_of(spins, row0, b) & jnp.int32(-(1 << 31) if b == 31 else 1 << b))
        state[0, pl.ds(row0, 8), :] = word

    def pack_side(group):
        row0 = pl.multiple_of(group * 8, 8)
        state[1, pl.ds(row0, 8), :] = shr(tile_of(spins, row0, tiles), jnp.int32(31)) | (
            tile_of(spins, row0, tiles + 1) & 2)

    groups = rows // 8
    halo = HALO // 8

    for copy in local:
        copy.wait()

    @pl.loop(halo, halo + groups)
    def _(group):
        pack_group(group)

    for copy in strips:
        copy.wait()
    first += [pass_on(stage, index) for stage in (0, 1) for index in (0, 1)]

    @pl.loop(0, packs * groups)
    def _(step):
        prepare(step // groups, halo + step % groups)

    @pl.loop(halo, halo + groups)
    def _(group):
        pack_side(group)

    @pl.loop(0, packs * groups)
    def _(step):
        prepare_side(step // groups, halo + step % groups)

    for copy in first:
        copy.wait()
    later = [step(stage, index) for stage in range(2, 1 + packs) for index in (0, 1) for step in (send, pass_on)]

    for group in (0, halo + groups):
        pack_group(group)
        pack_side(group)

    @pl.loop(0, 2)
    def _(side):
        prepare(0, side * (halo + groups))
        prepare_side(0, side * (halo + groups))

    lane = lax.broadcasted_iota(jnp.int32, (ext, LANES), 1)
    base = r * rows + c * cols - HALO
    site = lax.broadcasted_iota(jnp.int32, (ext, LANES), 0) + lane + base
    odd_sites = -(site & 1)

    def sweep(sweep_no):
        main, side = state[0], state[1]
        for colour_mask in (~odd_sites, odd_sites):
            across_m, across_s = lane_neighbours(main, side, lane)
            main, side = (
                updated(main, across_m, [accept[sweep_no, k, 0] for k in range(LEVELS)], colour_mask),
                updated(side, across_s, [accept[sweep_no, k, 1] for k in range(LEVELS)], colour_mask),
            )
        state[0] = main
        state[1] = side

    tile_id = lax.broadcasted_iota(jnp.int32, (WORD, LANES), 0)
    sub, lane8 = (lax.broadcasted_iota(jnp.int32, (HALO, LANES), d) for d in (0, 1))
    low_lanes = lane8 < LANES // 2
    near = (0, HALO - 1)
    side_rows = pl.ds(0, HALO)

    def places(depth):
        return (depth - 1, HALO - depth), (0, HALO - depth + 1), pl.ds(0, HALO + (depth - 1) * WORD)

    def send_edges(turn, depth):
        copies = []
        far, start, whole = places(depth)
        for index, (row0, dev) in enumerate(((HALO, up), (rows, down))):
            main, side = state[0, pl.ds(row0, HALO), :], state[1, pl.ds(row0, HALO), :]
            odd = odd_sites[row0:row0 + HALO]
            shift = (near[index] - far[index]) % HALO
            main = jnp.where(sub == near[index], (main & odd) | (pltpu.roll(main, shift, 0) & ~odd), main)
            for i in range(depth - 1):
                row = main[i + start[index]:i + start[index] + 1]
                bits = shr(jnp.broadcast_to(row, (WORD, LANES)), tile_id) & 1
                out_edge[turn, index, pl.ds(HALO + i * WORD, WORD), :] = bits
            out_edge[turn, index, side_rows, :] = jnp.where(low_lanes, shr(side, jnp.int32(1)), side) & 1
            copy = pltpu.make_async_remote_copy(
                src_ref=out_edge.at[turn, index, whole],
                dst_ref=in_edge.at[turn, index, whole],
                send_sem=edge_send.at[turn, index],
                recv_sem=edge_recv.at[turn, index],
                device_id=(dev, c),
                device_id_type=MESH,
            )
            copy.start()
            copies.append(copy)
        return copies

    def take_edges(turn, depth, copies):
        far, start, _ = places(depth)
        for index, (row0, copy) in enumerate(((HALO + rows, copies[0]), (0, copies[1]))):
            copy.wait()
            old = state[0, pl.ds(row0, HALO), :]
            odd = odd_sites[row0:row0 + HALO]
            word = old
            for i in range(depth - 1):
                bits = in_edge[turn, index, pl.ds(HALO + i * WORD, WORD), :] << tile_id
                row = bits[0:8] | bits[8:16] | bits[16:24] | bits[24:32]
                for shift in (4, 2, 1):
                    row = row | pltpu.roll(row, shift, 0)
                at = i + start[index]
                if at == near[index]:
                    word = jnp.where(sub == far[index], row, word)
                    row = (old & ~odd) | (row & odd)
                word = jnp.where(sub == at, row, word)
            state[0, pl.ds(row0, HALO), :] = word
            bits = in_edge[turn, index, side_rows, :]
            state[1, pl.ds(row0, HALO), :] = jnp.where(low_lanes, bits << 1, bits)

    for turn, depth in enumerate(DEPTHS):

        @pl.loop((done[turn] - depth) // 2, done[turn] // 2)
        def _(t):
            sweep(t)

        if turn + 1 < len(DEPTHS):
            copies = send_edges(turn, DEPTHS[turn + 1])
            if done[turn] == word_span:
                for copy in later:
                    copy.wait()

                @pl.loop(0, 2)
                def _(side):
                    prepare(1, side * (halo + groups))
                    prepare_side(1, side * (halo + groups))

            take_edges(turn, DEPTHS[turn + 1], copies)

    final = state[0, pl.ds(HALO, rows), :]
    word_ref[...] = final
    count[...] = lax.population_count(final)
    copies = []
    for k in range(1, n_cols):
        copy = pltpu.make_async_remote_copy(
            src_ref=count,
            dst_ref=peers.at[k - 1],
            send_sem=peer_send.at[k - 1],
            recv_sem=peer_recv.at[k - 1],
            device_id=(r, others[k - 1]),
            device_id_type=MESH,
        )
        copy.start()
        copies.append(copy)
    total = count[...]
    for k in range(1, n_cols):
        copies[k - 1].wait()
        total = total + peers[k - 1]
    downs = jnp.sum(total.astype(jnp.float32), axis=1, keepdims=True)
    width = n_cols * cols
    mean = (width - 2.0 * downs) / width
    at = lax.broadcasted_iota(jnp.int32, (rows, LANES), 0) == lax.broadcasted_iota(jnp.int32, (rows, LANES), 1)
    mean_ref[...] = jnp.sum(jnp.where(at, mean, 0.0), axis=0, keepdims=True)


def unpack_kernel(word_ref, row_ref, lattice_ref, mean_ref):
    word = word_ref[...]
    for b in range(lattice_ref.shape[1] // LANES):
        lattice_ref[:, b * LANES:(b + 1) * LANES] = 1 - ((shr(word, jnp.int32(b)) & 1) << 1)
    mean_ref[...] = row_ref[0, :mean_ref.shape[0]]


def on_device(shape, lattice, draws, thresholds):
    rows, cols = lattice.shape
    packs = draws.shape[0]
    assert cols == WORD * LANES and rows <= LANES and rows % 8 == 0 and sum(DEPTHS) == 2 * SWEEPS
    ext, wide = rows + 2 * HALO, cols + 2 * LANES
    n_cols = shape[1]
    turns = len(DEPTHS) - 1
    vmem, hbm = pltpu.VMEM, pl.ANY
    word, mean = pl.pallas_call(
        functools.partial(sweep_kernel, shape),
        out_shape=(
            jax.ShapeDtypeStruct((rows, LANES), jnp.int32),
            jax.ShapeDtypeStruct((1, LANES), jnp.float32),
        ),
        in_specs=[
            pl.BlockSpec(memory_space=hbm),
            pl.BlockSpec(memory_space=hbm),
            pl.BlockSpec(memory_space=pltpu.SMEM),
        ],
        out_specs=(pl.BlockSpec(memory_space=vmem), pl.BlockSpec(memory_space=vmem)),
        scratch_shapes=[
            vmem((ext, wide), jnp.int32),
            vmem((packs, ext, wide), jnp.int32),
            vmem((SWEEPS, LEVELS, 2, ext, LANES), jnp.int32),
            vmem((2, ext, LANES), jnp.int32),
            vmem((turns, 2, (max(DEPTHS) - 1) * WORD + HALO, LANES), jnp.int32),
            vmem((turns, 2, (max(DEPTHS) - 1) * WORD + HALO, LANES), jnp.int32),
            vmem((rows, LANES), jnp.int32),
            vmem((n_cols - 1, rows, LANES), jnp.int32),
            pltpu.SemaphoreType.DMA((1 + packs,)),
            pltpu.SemaphoreType.DMA((1 + packs, 8)),
            pltpu.SemaphoreType.DMA((1 + packs, 8)),
            pltpu.SemaphoreType.DMA((turns, 2)),
            pltpu.SemaphoreType.DMA((turns, 2)),
            pltpu.SemaphoreType.DMA((n_cols - 1,)),
            pltpu.SemaphoreType.DMA((n_cols - 1,)),
        ],
        compiler_params=pltpu.CompilerParams(collective_id=0, has_side_effects=True),
        name="sweeps",
    )(lattice, draws, thresholds)
    final, means = pl.pallas_call(
        unpack_kernel,
        out_shape=(
            jax.ShapeDtypeStruct((rows, cols), jnp.int32),
            jax.ShapeDtypeStruct((rows,), jnp.float32),
        ),
        name="unpack",
    )(word, mean)
    return final, means


def solution(mesh):
    shape = (mesh.shape["rows"], mesh.shape["cols"])
    in_specs = (P("rows", "cols"), P(None, "rows", "cols"), P())
    out_specs = (P("rows", "cols"), P("rows"))
    return jax.shard_map(
        functools.partial(on_device, shape), mesh=mesh, in_specs=in_specs, out_specs=out_specs, check_vma=False
    )
```

```python
import functools

import jax
import jax.numpy as jnp
from jax import lax
from jax.experimental import pallas as pl
from jax.experimental.pallas import tpu as pltpu
from jax.sharding import PartitionSpec as P

SWEEPS = 8
LEVELS = 5
PER_WORD = 4
BITS = 8
DEPTHS = (4, 4, 8)
HALO = 8
LANES = 128
WORD = 32
MESH = pl.DeviceIdType.MESH

shr = lax.shift_right_logical


def transposed(words):
    words = list(words)
    mask = 0x0000FFFF
    j = 16
    while j:
        signed = mask - (1 << 32) if mask >> 31 else mask
        for k in range(WORD):
            if k & j:
                continue
            low, high = words[k], words[k + j]
            t = (shr(low, jnp.int32(j)) ^ high) & jnp.int32(signed)
            words[k + j] = high ^ t
            words[k] = low ^ (t << j)
        j >>= 1
        mask = (mask ^ (mask << j)) & 0xFFFFFFFF
    return words


def accept_masks(planes, bit_masks):
    below = []
    for level in range(LEVELS):
        t = bit_masks[level]
        z = planes[0] & t[0]
        for b in range(1, BITS):
            z = (z ^ (t[b - 1] ^ t[b])) & (planes[b] ^ ~t[b])
        below.append((z ^ t[BITS - 1]) | t[BITS])
    return below[0], below[0] ^ below[1], below[2], below[2] ^ below[3], below[0] ^ below[4]


def lane_neighbours(main, side, lane):
    rm, rs = pltpu.roll(main, 1, 1), pltpu.roll(side, 1, 1)
    sm, ss = pltpu.roll(main, LANES - 1, 1), pltpu.roll(side, LANES - 1, 1)
    first, last = lane == 0, lane == LANES - 1
    left_m = jnp.where(first, (rm << 1) | (rs & 1), rm)
    left_s = jnp.where(first, shr(rm, jnp.int32(30)) & 2, rs)
    right_m = jnp.where(last, shr(sm, jnp.int32(1)) | ((ss & 2) << 30), sm)
    right_s = jnp.where(last, sm & 1, ss)
    return (left_m, right_m), (left_s, right_s)


def updated(word, across, accept, colour_mask):
    rows = word.shape[0]
    a0, d1, a2, d3, d4 = accept
    x1, x2 = pltpu.roll(word, 1, 0) ^ word, pltpu.roll(word, rows - 1, 0) ^ word
    x3, x4 = across[0] ^ word, across[1] ^ word
    p, c1 = x1 ^ x2, ~(x1 | x2)
    q, c2 = x3 ^ x4, ~(x3 | x4)
    ones, twos, fours = p ^ q, (c1 ^ c2) | (p & q), c1 & c2
    low, high = a0 ^ (ones & d1), a2 ^ (ones & d3)
    take = low ^ (twos & (low ^ high)) ^ (fours & d4)
    return word ^ (take & colour_mask)


def sweep_kernel(shape, lat_ref, draws_ref, thr_ref, word_ref, mean_ref,
                 spins, draws, accept, state, out_edge, in_edge, count, peers,
                 local_sem, send_sem, recv_sem, edge_send, edge_recv, peer_send, peer_recv):
    n_rows, n_cols = shape
    rows, cols = lat_ref.shape
    tiles = cols // LANES
    packs = draws_ref.shape[0]
    ext = rows + 2 * HALO
    r, c = lax.axis_index("rows"), lax.axis_index("cols")
    up, down = lax.rem(r + n_rows - 1, n_rows), lax.rem(r + 1, n_rows)
    left, right = lax.rem(c + n_cols - 1, n_cols), lax.rem(c + 1, n_cols)

    local = [pltpu.make_async_copy(lat_ref, spins.at[pl.ds(HALO, rows), pl.ds(0, cols)], local_sem.at[0])]
    for pack in range(packs):
        local.append(pltpu.make_async_copy(
            draws_ref.at[pack], draws.at[pack, pl.ds(HALO, rows), pl.ds(0, cols)], local_sem.at[1 + pack]))
    for copy in local:
        copy.start()

    barrier = pltpu.get_barrier_semaphore()
    around = [(up, c), (down, c), (r, left), (r, right)]
    others = [lax.rem(c + k, n_cols) for k in range(1, n_cols)]
    for target in around + [(r, b) for b in others[1:-1]]:
        pl.semaphore_signal(barrier, inc=1, device_id=target, device_id_type=MESH)
    pl.semaphore_wait(barrier, len(around) + n_cols - 3)

    def row_part(depth):
        return {-1: (0, depth, HALO + rows), 0: (0, rows, HALO), 1: (rows - depth, depth, HALO - depth)}

    col_part = {-1: (0, LANES, cols + LANES), 0: (0, cols, 0), 1: (cols - LANES, LANES, cols)}
    row_id = {-1: up, 0: r, 1: down}
    col_id = {-1: left, 0: c, 1: right}
    sides = [(-1, 0), (1, 0), (0, -1), (0, 1)]
    done = [sum(DEPTHS[:turn + 1]) for turn in range(len(DEPTHS))]
    word_span = 2 * PER_WORD
    reach = [DEPTHS[0]] + [
        max(d for d, end in zip(DEPTHS, done) if end - d < word_span * (p + 1) and end > word_span * p) - 1
        for p in range(packs)
    ]

    def send(stage, index):
        dr, dc = sides[index]
        r0, rn, rd = row_part(reach[stage])[dr]
        c0, cn, cd = col_part[dc]
        src, dst = (lat_ref, spins) if stage == 0 else (draws_ref.at[stage - 1], draws.at[stage - 1])
        copy = pltpu.make_async_remote_copy(
            src_ref=src.at[pl.ds(r0, rn), pl.ds(c0, cn)],
            dst_ref=dst.at[pl.ds(rd, rn), pl.ds(cd, cn)],
            send_sem=send_sem.at[stage, index],
            recv_sem=recv_sem.at[stage, index],
            device_id=(row_id[dr], col_id[dc]),
            device_id_type=MESH,
        )
        copy.start()
        return copy

    def pass_on(stage, index):
        r0, rn, rd = row_part(reach[stage])[sides[index][0]]
        block = spins if stage == 0 else draws.at[stage - 1]
        copy = pltpu.make_async_remote_copy(
            src_ref=block.at[pl.ds(HALO + r0, rn), pl.ds(cols, 2 * LANES)],
            dst_ref=block.at[pl.ds(rd, rn), pl.ds(cols, 2 * LANES)],
            send_sem=send_sem.at[stage, 4 + index],
            recv_sem=recv_sem.at[stage, 4 + index],
            device_id=(row_id[sides[index][0]], c),
            device_id_type=MESH,
        )
        copy.start()
        return copy

    first = [send(stage, index) for stage in (0, 1) for index in (0, 1)]
    strips = [send(stage, index) for stage in range(1 + packs) for index in (2, 3)]

    bit_masks = []
    for level in range(LEVELS):
        t = thr_ref[level]
        bit_masks.append([-((t >> b) & 1) for b in range(BITS + 1)])

    def tile_of(ref, row0, b):
        return ref[pl.ds(row0, 8), pl.ds(b * LANES, LANES)]

    def prepare(pack, group):
        row0 = pl.multiple_of(group * 8, 8)
        source = draws.at[pack]
        planes = transposed([tile_of(source, row0, b) for b in range(tiles)])
        for t in range(PER_WORD):
            masks = accept_masks(planes[BITS * t:BITS * (t + 1)], bit_masks)
            for k in range(LEVELS):
                accept[pack * PER_WORD + t, k, 0, pl.ds(row0, 8), :] = masks[k]

    def prepare_side(pack, group):
        row0 = pl.multiple_of(group * 8, 8)
        source = draws.at[pack]
        lo, hi = tile_of(source, row0, tiles), tile_of(source, row0, tiles + 1)
        even = (lo & 0x55555555) | ((hi & 0x55555555) << 1)
        odd = (shr(lo, jnp.int32(1)) & 0x55555555) | (hi & -0x55555556)
        planes = [shr((even, odd)[q & 1], jnp.int32(q & ~1)) for q in range(WORD)]
        for t in range(PER_WORD):
            masks = accept_masks(planes[BITS * t:BITS * (t + 1)], bit_masks)
            for k in range(LEVELS):
                accept[pack * PER_WORD + t, k, 1, pl.ds(row0, 8), :] = masks[k]

    def pack_group(group):
        row0 = pl.multiple_of(group * 8, 8)
        word = shr(tile_of(spins, row0, 0), jnp.int32(31))
        for b in range(1, tiles):
            word = word | (tile_of(spins, row0, b) & jnp.int32(-(1 << 31) if b == 31 else 1 << b))
        state[0, pl.ds(row0, 8), :] = word

    def pack_side(group):
        row0 = pl.multiple_of(group * 8, 8)
        state[1, pl.ds(row0, 8), :] = shr(tile_of(spins, row0, tiles), jnp.int32(31)) | (
            tile_of(spins, row0, tiles + 1) & 2)

    groups = rows // 8
    halo = HALO // 8

    for copy in local:
        copy.wait()

    @pl.loop(halo, halo + groups)
    def _(group):
        pack_group(group)

    for copy in strips:
        copy.wait()
    first += [pass_on(stage, index) for stage in (0, 1) for index in (0, 1)]
    later = [step(stage, index) for stage in range(2, 1 + packs) for index in (0, 1) for step in (send, pass_on)]

    @pl.loop(0, packs * groups)
    def _(step):
        prepare(step // groups, halo + step % groups)

    @pl.loop(halo, halo + groups)
    def _(group):
        pack_side(group)

    @pl.loop(0, packs * groups)
    def _(step):
        prepare_side(step // groups, halo + step % groups)

    for copy in first:
        copy.wait()

    for group in (0, halo + groups):
        pack_group(group)
        pack_side(group)

    @pl.loop(0, 2)
    def _(side):
        prepare(0, side * (halo + groups))
        prepare_side(0, side * (halo + groups))

    lane = lax.broadcasted_iota(jnp.int32, (ext, LANES), 1)
    base = r * rows + c * cols - HALO
    site = lax.broadcasted_iota(jnp.int32, (ext, LANES), 0) + lane + base
    odd_sites = -(site & 1)

    def sweep(sweep_no):
        main, side = state[0], state[1]
        for colour_mask in (~odd_sites, odd_sites):
            across_m, across_s = lane_neighbours(main, side, lane)
            main, side = (
                updated(main, across_m, [accept[sweep_no, k, 0] for k in range(LEVELS)], colour_mask),
                updated(side, across_s, [accept[sweep_no, k, 1] for k in range(LEVELS)], colour_mask),
            )
        state[0] = main
        state[1] = side

    tile_id = lax.broadcasted_iota(jnp.int32, (WORD, LANES), 0)
    sub, lane8 = (lax.broadcasted_iota(jnp.int32, (HALO, LANES), d) for d in (0, 1))
    low_lanes = lane8 < LANES // 2
    near = (0, HALO - 1)
    side_rows = pl.ds(0, HALO)

    def places(depth):
        return (depth - 1, HALO - depth), (0, HALO - depth + 1), pl.ds(0, HALO + (depth - 1) * WORD)

    def send_edges(turn, depth):
        copies = []
        far, start, whole = places(depth)
        for index, (row0, dev) in enumerate(((HALO, up), (rows, down))):
            main, side = state[0, pl.ds(row0, HALO), :], state[1, pl.ds(row0, HALO), :]
            odd = odd_sites[row0:row0 + HALO]
            shift = (near[index] - far[index]) % HALO
            main = jnp.where(sub == near[index], (main & odd) | (pltpu.roll(main, shift, 0) & ~odd), main)
            for i in range(depth - 1):
                row = main[i + start[index]:i + start[index] + 1]
                bits = shr(jnp.broadcast_to(row, (WORD, LANES)), tile_id) & 1
                out_edge[turn, index, pl.ds(HALO + i * WORD, WORD), :] = bits
            out_edge[turn, index, side_rows, :] = jnp.where(low_lanes, shr(side, jnp.int32(1)), side) & 1
            copy = pltpu.make_async_remote_copy(
                src_ref=out_edge.at[turn, index, whole],
                dst_ref=in_edge.at[turn, index, whole],
                send_sem=edge_send.at[turn, index],
                recv_sem=edge_recv.at[turn, index],
                device_id=(dev, c),
                device_id_type=MESH,
            )
            copy.start()
            copies.append(copy)
        return copies

    def take_edges(turn, depth, copies):
        far, start, _ = places(depth)
        for index, (row0, copy) in enumerate(((HALO + rows, copies[0]), (0, copies[1]))):
            copy.wait()
            old = state[0, pl.ds(row0, HALO), :]
            odd = odd_sites[row0:row0 + HALO]
            word = old
            for i in range(depth - 1):
                bits = in_edge[turn, index, pl.ds(HALO + i * WORD, WORD), :] << tile_id
                row = bits[0:8] | bits[8:16] | bits[16:24] | bits[24:32]
                for shift in (4, 2, 1):
                    row = row | pltpu.roll(row, shift, 0)
                at = i + start[index]
                if at == near[index]:
                    word = jnp.where(sub == far[index], row, word)
                    row = (old & ~odd) | (row & odd)
                word = jnp.where(sub == at, row, word)
            state[0, pl.ds(row0, HALO), :] = word
            bits = in_edge[turn, index, side_rows, :]
            state[1, pl.ds(row0, HALO), :] = jnp.where(low_lanes, bits << 1, bits)

    for turn, depth in enumerate(DEPTHS):

        @pl.loop((done[turn] - depth) // 2, done[turn] // 2)
        def _(t):
            sweep(t)

        if turn + 1 < len(DEPTHS):
            copies = send_edges(turn, DEPTHS[turn + 1])
            if done[turn] == word_span:
                for copy in later:
                    copy.wait()

                @pl.loop(0, 2)
                def _(side):
                    prepare(1, side * (halo + groups))
                    prepare_side(1, side * (halo + groups))

            take_edges(turn, DEPTHS[turn + 1], copies)

    final = state[0, pl.ds(HALO, rows), :]
    word_ref[...] = final
    count[...] = lax.population_count(final)
    copies = []
    for k in range(1, n_cols):
        copy = pltpu.make_async_remote_copy(
            src_ref=count,
            dst_ref=peers.at[k - 1],
            send_sem=peer_send.at[k - 1],
            recv_sem=peer_recv.at[k - 1],
            device_id=(r, others[k - 1]),
            device_id_type=MESH,
        )
        copy.start()
        copies.append(copy)
    total = count[...]
    for k in range(1, n_cols):
        copies[k - 1].wait()
        total = total + peers[k - 1]
    downs = jnp.sum(total.astype(jnp.float32), axis=1, keepdims=True)
    width = n_cols * cols
    mean = (width - 2.0 * downs) / width
    at = lax.broadcasted_iota(jnp.int32, (rows, LANES), 0) == lax.broadcasted_iota(jnp.int32, (rows, LANES), 1)
    mean_ref[...] = jnp.sum(jnp.where(at, mean, 0.0), axis=0, keepdims=True)


def unpack_kernel(word_ref, row_ref, lattice_ref, mean_ref):
    word = word_ref[...]
    for b in range(lattice_ref.shape[1] // LANES):
        lattice_ref[:, b * LANES:(b + 1) * LANES] = 1 - ((shr(word, jnp.int32(b)) & 1) << 1)
    mean_ref[...] = row_ref[0, :mean_ref.shape[0]]


def on_device(shape, lattice, draws, thresholds):
    rows, cols = lattice.shape
    packs = draws.shape[0]
    assert cols == WORD * LANES and rows <= LANES and rows % 8 == 0 and sum(DEPTHS) == 2 * SWEEPS
    ext, wide = rows + 2 * HALO, cols + 2 * LANES
    n_cols = shape[1]
    turns = len(DEPTHS) - 1
    vmem, hbm = pltpu.VMEM, pl.ANY
    word, mean = pl.pallas_call(
        functools.partial(sweep_kernel, shape),
        out_shape=(
            jax.ShapeDtypeStruct((rows, LANES), jnp.int32),
            jax.ShapeDtypeStruct((1, LANES), jnp.float32),
        ),
        in_specs=[
            pl.BlockSpec(memory_space=hbm),
            pl.BlockSpec(memory_space=hbm),
            pl.BlockSpec(memory_space=pltpu.SMEM),
        ],
        out_specs=(pl.BlockSpec(memory_space=vmem), pl.BlockSpec(memory_space=vmem)),
        scratch_shapes=[
            vmem((ext, wide), jnp.int32),
            vmem((packs, ext, wide), jnp.int32),
            vmem((SWEEPS, LEVELS, 2, ext, LANES), jnp.int32),
            vmem((2, ext, LANES), jnp.int32),
            vmem((turns, 2, (max(DEPTHS) - 1) * WORD + HALO, LANES), jnp.int32),
            vmem((turns, 2, (max(DEPTHS) - 1) * WORD + HALO, LANES), jnp.int32),
            vmem((rows, LANES), jnp.int32),
            vmem((n_cols - 1, rows, LANES), jnp.int32),
            pltpu.SemaphoreType.DMA((1 + packs,)),
            pltpu.SemaphoreType.DMA((1 + packs, 8)),
            pltpu.SemaphoreType.DMA((1 + packs, 8)),
            pltpu.SemaphoreType.DMA((turns, 2)),
            pltpu.SemaphoreType.DMA((turns, 2)),
            pltpu.SemaphoreType.DMA((n_cols - 1,)),
            pltpu.SemaphoreType.DMA((n_cols - 1,)),
        ],
        compiler_params=pltpu.CompilerParams(collective_id=0, has_side_effects=True),
        name="sweeps",
    )(lattice, draws, thresholds)
    final, means = pl.pallas_call(
        unpack_kernel,
        out_shape=(
            jax.ShapeDtypeStruct((rows, cols), jnp.int32),
            jax.ShapeDtypeStruct((rows,), jnp.float32),
        ),
        name="unpack",
    )(word, mean)
    return final, means


def solution(mesh):
    shape = (mesh.shape["rows"], mesh.shape["cols"])
    in_specs = (P("rows", "cols"), P(None, "rows", "cols"), P())
    out_specs = (P("rows", "cols"), P("rows"))
    return jax.shard_map(
        functools.partial(on_device, shape), mesh=mesh, in_specs=in_specs, out_specs=out_specs, check_vma=False
    )
```
